32 devices in a mesh: shot: 4 (over x, core), tile: 8 (over z, y).
Axes of the slice: x: 2, y: 2, z: 4, core: 2. Of those that a mesh axis runs over, the one named last changes fastest.
Arguments:
- partials: bfloat16 [32, 8, 512, 512], P(('shot', 'tile')), may hold values from -6 to 6
Outputs:
- filtered: float32 [8, 512, 512], P('shot', 'tile')
The draws below stay inside these ranges and needn't reach their ends.
All inputs are finite; a program needn't handle non-finite values.
Results may differ from the reference program's by a relative error of at most 0.0003.
Values may be sent and summed in bfloat16 or wider, within the bound.
No kernel may reach another device: no remote copies, remote signals or barrier semaphores. Data moves between devices by JAX's collectives and lax.ppermute only.
A program may use at most 64 MiB of HBM per device.

```python
import jax
import jax.numpy as jnp
from jax import lax

DEPTH = 8
NX = 512
NY = 512
SHOTS = 32


def block_scale(key, shape, shards, low, high):
    level = 1.0
    for dim, blocks in shards:
        draws = jax.random.uniform(jax.random.fold_in(jax.random.fold_in(key, 6), dim), (blocks,), jnp.float32, low / len(shards), high / len(shards))
        level = level * jnp.repeat(jnp.exp(draws), shape[dim] // blocks).reshape((-1,) + (1,) * (len(shape) - 1 - dim))
    return level


def gaussian(own_key, extent, spread, bound, pieces=(), kind=jnp.bfloat16):
    result = jax.random.normal(own_key, extent, jnp.float32) * spread
    if len(pieces) > 0:
        result = block_scale(own_key, extent, pieces, -0.22, 0.18) * result
    return jnp.clip(result, min=-bound, max=bound).astype(kind)


def setup_inputs(seed: int = 0) -> dict:
    splits = jax.random.split(jax.random.key(seed), 2)
    return {
        "partials": gaussian(splits[0], (SHOTS, DEPTH, NX, NY), 1.0, 6.0, ((0, 32),)),
    }


def reference(partials):

    def add_one(total, piece):
        return (total + piece.astype(jnp.float32), None)
    start = jnp.zeros((DEPTH, NX, NY), jnp.float32)
    stack, unused = lax.scan(add_one, start, partials)
    image = stack / jnp.sqrt(jnp.float32(SHOTS))
    padded = jnp.pad(image, 1)
    beside = padded[2:, 1:-1, 1:-1] + padded[:-2, 1:-1, 1:-1]
    beside = beside + padded[1:-1, 2:, 1:-1] + padded[1:-1, :-2, 1:-1]
    beside = beside + padded[1:-1, 1:-1, 2:] + padded[1:-1, 1:-1, :-2]
    return 6.0 * image - beside
```

```python
import jax
import jax.numpy as jnp
from jax import lax
from jax.sharding import PartitionSpec as P


def bits_of(count):
    return count.bit_length() - 1


def halve(block, labels, step):
    axis, bit = step
    count = lax.axis_size(axis)
    dim = labels.index(step)
    mine = (lax.axis_index(axis) >> bit) & 1
    keep = lax.dynamic_index_in_dim(block, mine, dim, keepdims=False)
    send = lax.dynamic_index_in_dim(block, 1 - mine, dim, keepdims=False)
    got = lax.ppermute(send, axis, [(i, i ^ (1 << bit)) for i in range(count)])
    total = keep.astype(jnp.float32) + got.astype(jnp.float32)
    return total, labels[:dim] + labels[dim + 1 :]


def shifted(cells, axis, dim):
    count = lax.axis_size(axis)
    size = cells.shape[dim]
    head = lax.slice_in_dim(cells, 0, 1, axis=dim)
    tail = lax.slice_in_dim(cells, size - 1, size, axis=dim)
    before = lax.ppermute(tail, axis, [(i, i + 1) for i in range(count - 1)])
    after = lax.ppermute(head, axis, [(i + 1, i) for i in range(count - 1)])
    return before, after


def body(partials):
    groups = lax.axis_size("shot")
    members = lax.axis_size("tile")
    shots, depth, nx, ny = partials.shape
    part = depth // groups
    rows = nx // members
    sbits = [("shot", b) for b in reversed(range(bits_of(groups)))]
    tbits = [("tile", b) for b in reversed(range(bits_of(members)))]
    view = partials.reshape((2,) * len(sbits) + (part,) + (2,) * len(tbits) + (rows, ny))
    labels = sbits + ["part"] + tbits + ["rows", "ny"]
    chip = [("shot", 0)]
    across = [s for s in sbits if s not in chip]
    near = [("tile", 0)]
    line = [("tile", b) for b in range(1, len(tbits))]
    orders = (across + chip + near + line, near + chip + across + line)
    colors = 2 if part % 2 == 0 else 1
    pieces = []
    for c in range(colors):
        block = lax.slice_in_dim(view, c * part // colors, (c + 1) * part // colors, axis=len(sbits))
        left = labels
        for step in orders[c]:
            block, left = halve(block, left, step)
        pieces.append(block)
    image = jnp.concatenate(pieces, axis=0) * (1.0 / jnp.sqrt(jnp.float32(groups * members)))
    above, below = shifted(image, "shot", 0)
    north, south = shifted(image, "tile", 1)
    deep = jnp.concatenate([above, image, below], axis=0)
    beside = deep[2:] + deep[:-2]
    wide = jnp.concatenate([north, image, south], axis=1)
    beside = beside + wide[:, 2:] + wide[:, :-2]
    long = jnp.pad(image, ((0, 0), (0, 0), (1, 1)))
    beside = beside + long[:, :, 2:] + long[:, :, :-2]
    return 6.0 * image - beside


def solution(mesh):
    return jax.shard_map(
        body,
        mesh=mesh,
        in_specs=(P(("shot", "tile"), None, None, None),),
        out_specs=P("shot", "tile", None),
        check_vma=False,
    )
```

```python
import jax
import jax.numpy as jnp
from jax import lax
from jax.experimental import pallas as pl
from jax.experimental.pallas import tpu as pltpu
from jax.sharding import PartitionSpec as P


COLORS = 2


def bits_of(count):
    return count.bit_length() - 1


def halve(block, labels, step):
    axis, bit = step
    count = lax.axis_size(axis)
    dim = labels.index(step)
    mine = (lax.axis_index(axis) >> bit) & 1
    keep = lax.dynamic_index_in_dim(block, mine, dim, keepdims=False)
    send = lax.dynamic_index_in_dim(block, 1 - mine, dim, keepdims=False)
    got = lax.ppermute(send, axis, [(i, i ^ (1 << bit)) for i in range(count)])
    total = keep.astype(jnp.float32) + got.astype(jnp.float32)
    return total, labels[:dim] + labels[dim + 1 :]


def filter_pair(own, other, core, groups, scale):
    depth, nx, ny = own.shape
    part = depth // groups
    chunk = 64
    edge = 8

    def plane(h, j, core):
        return (2 * h + core[0]) * part + j

    def kernel(core, om, oc, op, pm, pc, pp, out, pad):
        d = plane(pl.program_id(0), pl.program_id(1), core)
        low = jnp.where(d > 0, scale, 0.0)
        high = jnp.where(d < depth - 1, scale, 0.0)
        zeros = jnp.zeros((edge, ny), jnp.float32)
        pad[pl.ds(0, edge)] = zeros
        pad[pl.ds(edge + nx, edge)] = zeros
        for r in range(0, nx, chunk):
            rows = pl.ds(r, chunk)
            both = oc[0, rows].astype(jnp.float32) + pc[0, rows].astype(jnp.float32)
            pad[pl.ds(edge + r, chunk)] = both * scale
        lane = lax.broadcasted_iota(jnp.int32, (chunk, ny), 1)
        for r in range(0, nx, chunk):
            rows = pl.ds(r, chunk)
            mid = pad[pl.ds(edge + r, chunk)]
            beside = (om[0, rows].astype(jnp.float32) + pm[0, rows].astype(jnp.float32)) * low
            beside = beside + (op[0, rows].astype(jnp.float32) + pp[0, rows].astype(jnp.float32)) * high
            beside = beside + pad[pl.ds(edge + r - 1, chunk)] + pad[pl.ds(edge + r + 1, chunk)]
            beside = beside + jnp.where(lane > 0, pltpu.roll(mid, 1, 1), 0.0)
            beside = beside + jnp.where(lane < ny - 1, pltpu.roll(mid, ny - 1, 1), 0.0)
            out[0, 0, rows] = 6.0 * mid - beside

    def spec(shift):
        def index(h, j, core):
            return (jnp.clip(plane(h, j, core) + shift, 0, depth - 1), 0, 0)

        return pl.BlockSpec((1, nx, ny), index)

    specs = [spec(-1), spec(0), spec(1)]
    return pl.pallas_call(
        kernel,
        grid_spec=pltpu.PrefetchScalarGridSpec(
            num_scalar_prefetch=1,
            grid=(groups // 2, part),
            in_specs=specs + specs,
            out_specs=pl.BlockSpec((1, 1, nx, ny), lambda h, j, core: (h, j, 0, 0)),
            scratch_shapes=[pltpu.VMEM((nx + 2 * edge, ny), jnp.float32)],
        ),
        out_shape=jax.ShapeDtypeStruct((groups // 2, part, nx, ny), jnp.float32),
        name="filter_pair",
    )(core, own, own, own, other, other, other)


def body(partials):
    groups = lax.axis_size("shot")
    members = lax.axis_size("tile")
    shots, depth, nx, ny = partials.shape
    part = depth // groups
    rows = nx // members
    own = partials[0]
    other = lax.ppermute(own, "shot", [(i, i ^ 1) for i in range(groups)])
    core = (lax.axis_index("shot") & 1).reshape(1)
    scale = 1.0 / float(groups * members) ** 0.5
    pair = filter_pair(own, other, core, groups, scale)
    sbits = [("shot", b) for b in reversed(range(1, bits_of(groups)))]
    tbits = [("tile", b) for b in reversed(range(bits_of(members)))]
    view = pair.reshape((2,) * len(sbits) + (part,) + (2,) * len(tbits) + (rows, ny))
    labels = sbits + ["part"] + tbits + ["rows", "ny"]
    steps = sbits[::-1] + tbits[::-1]
    first, rest = steps[:3], steps[3:]
    units = rows // 8
    colors = min(COLORS, units)
    cuts = [8 * ((units * c + colors // 2) // colors) for c in range(colors + 1)]
    cuts[-1] = rows
    pieces = [
        (lax.slice_in_dim(view, cuts[c], cuts[c + 1], axis=len(labels) - 2), labels)
        for c in range(colors)
    ]
    for k in range(len(steps)):
        for c in range(colors):
            order = first[c:] + first[:c] + rest
            pieces[c] = halve(*pieces[c], order[k])
    return jnp.concatenate([block for block, left in pieces], axis=1)


def solution(mesh):
    return jax.shard_map(
        body,
        mesh=mesh,
        in_specs=(P(("shot", "tile"), None, None, None),),
        out_specs=P("shot", "tile", None),
        check_vma=False,
    )
```

```python
import jax
import jax.numpy as jnp
from jax import lax
from jax.experimental import pallas as pl
from jax.experimental.pallas import tpu as pltpu
from jax.sharding import PartitionSpec as P


COLORS = 2


def bits_of(count):
    return count.bit_length() - 1


def halve(block, labels, step):
    axis, bit = step
    count = lax.axis_size(axis)
    dim = labels.index(step)
    mine = (lax.axis_index(axis) >> bit) & 1
    keep = lax.dynamic_index_in_dim(block, mine, dim, keepdims=False)
    send = lax.dynamic_index_in_dim(block, 1 - mine, dim, keepdims=False)
    got = lax.ppermute(send, axis, [(i, i ^ (1 << bit)) for i in range(count)])
    total = keep.astype(jnp.float32) + got.astype(jnp.float32)
    return total, labels[:dim] + labels[dim + 1 :]


def filter_pair(own, other, core, groups, scale):
    depth, nx, ny = own.shape
    part = depth // groups
    chunk = 64
    edge = 8

    def kernel(core, om, oc, op, pm, pc, pp, out, pad):
        block = 2 * pl.program_id(0) + core[0]
        low = jnp.where(block > 0, scale, 0.0)
        high = jnp.where(block < groups - 1, scale, 0.0)
        zeros = jnp.zeros((edge, ny), jnp.float32)
        pad[pl.ds(0, edge)] = zeros
        pad[pl.ds(edge + nx, edge)] = zeros
        lane = lax.broadcasted_iota(jnp.int32, (chunk, ny), 1)

        def both(own_ref, other_ref, level, rows, factor):
            left = own_ref[level, rows].astype(jnp.float32)
            return (left + other_ref[level, rows].astype(jnp.float32)) * factor

        for j in range(part):
            for r in range(0, nx, chunk):
                pad[pl.ds(edge + r, chunk)] = both(oc, pc, j, pl.ds(r, chunk), scale)
            for r in range(0, nx, chunk):
                rows = pl.ds(r, chunk)
                mid = pad[pl.ds(edge + r, chunk)]
                beside = both(om, pm, 0, rows, low) if j == 0 else both(oc, pc, j - 1, rows, scale)
                beside = beside + (both(op, pp, 0, rows, high) if j == part - 1 else both(oc, pc, j + 1, rows, scale))
                beside = beside + pad[pl.ds(edge + r - 1, chunk)] + pad[pl.ds(edge + r + 1, chunk)]
                beside = beside + jnp.where(lane > 0, pltpu.roll(mid, 1, 1), 0.0)
                beside = beside + jnp.where(lane < ny - 1, pltpu.roll(mid, ny - 1, 1), 0.0)
                out[0, j, rows] = 6.0 * mid - beside

    def outer(shift):
        def index(h, core):
            return (jnp.clip((2 * h + core[0]) * part + shift, 0, depth - 1), 0, 0)

        return pl.BlockSpec((1, nx, ny), index)

    centre = pl.BlockSpec((part, nx, ny), lambda h, core: (2 * h + core[0], 0, 0))
    specs = [outer(-1), centre, outer(part)]
    return pl.pallas_call(
        kernel,
        grid_spec=pltpu.PrefetchScalarGridSpec(
            num_scalar_prefetch=1,
            grid=(groups // 2,),
            in_specs=specs + specs,
            out_specs=pl.BlockSpec((1, part, nx, ny), lambda h, core: (h, 0, 0, 0)),
            scratch_shapes=[pltpu.VMEM((nx + 2 * edge, ny), jnp.float32)],
        ),
        out_shape=jax.ShapeDtypeStruct((groups // 2, part, nx, ny), jnp.float32),
        name="filter_pair",
    )(core, own, own, own, other, other, other)


def body(partials):
    groups = lax.axis_size("shot")
    members = lax.axis_size("tile")
    shots, depth, nx, ny = partials.shape
    part = depth // groups
    rows = nx // members
    own = partials[0]
    other = lax.ppermute(own, "shot", [(i, i ^ 1) for i in range(groups)])
    core = (lax.axis_index("shot") & 1).reshape(1)
    scale = 1.0 / float(groups * members) ** 0.5
    pair = filter_pair(own, other, core, groups, scale)
    sbits = [("shot", b) for b in reversed(range(1, bits_of(groups)))]
    tbits = [("tile", b) for b in reversed(range(bits_of(members)))]
    view = pair.reshape((2,) * len(sbits) + (part,) + (2,) * len(tbits) + (rows, ny))
    labels = sbits + ["part"] + tbits + ["rows", "ny"]
    steps = sbits[::-1] + tbits[::-1]
    first, rest = steps[:3], steps[3:]
    colors = COLORS if part % COLORS == 0 else 1
    cuts = [part * c // colors for c in range(colors + 1)]
    pieces = [
        (lax.slice_in_dim(view, cuts[c], cuts[c + 1], axis=len(sbits)), labels)
        for c in range(colors)
    ]
    for k in range(len(steps)):
        for c in range(colors):
            order = first[c:] + first[:c] + rest
            pieces[c] = halve(*pieces[c], order[k])
    return jnp.concatenate([block for block, left in pieces], axis=0)


def solution(mesh):
    return jax.shard_map(
        body,
        mesh=mesh,
        in_specs=(P(("shot", "tile"), None, None, None),),
        out_specs=P("shot", "tile", None),
        check_vma=False,
    )
```

```python
import jax
import jax.numpy as jnp
from jax import lax
from jax.experimental import pallas as pl
from jax.experimental.pallas import tpu as pltpu
from jax.sharding import PartitionSpec as P


def bits_of(count):
    return count.bit_length() - 1


def halve(block, labels, step):
    axis, bit = step
    count = lax.axis_size(axis)
    dim = labels.index(step)
    mine = (lax.axis_index(axis) >> bit) & 1
    keep = lax.dynamic_index_in_dim(block, mine, dim, keepdims=False)
    send = lax.dynamic_index_in_dim(block, 1 - mine, dim, keepdims=False)
    got = lax.ppermute(send, axis, [(i, i ^ (1 << bit)) for i in range(count)])
    total = keep.astype(jnp.float32) + got.astype(jnp.float32)
    return total, labels[:dim] + labels[dim + 1 :]


def filter_pair(own, other, core, groups, scale):
    depth, nx, ny = own.shape
    part = depth // groups
    chunk = 64
    edge = 8

    def kernel(core, om, oc, op, pm, pc, pp, *rest):
        outs, pad = rest[:-1], rest[-1]
        block = 2 * pl.program_id(0) + core[0]
        low = jnp.where(block > 0, scale, 0.0)
        high = jnp.where(block < groups - 1, scale, 0.0)
        zeros = jnp.zeros((edge, ny), jnp.float32)
        pad[pl.ds(0, edge)] = zeros
        pad[pl.ds(edge + nx, edge)] = zeros
        lane = lax.broadcasted_iota(jnp.int32, (chunk, ny), 1)

        def both(own_ref, other_ref, level, rows, factor):
            left = own_ref[level, rows].astype(jnp.float32)
            return (left + other_ref[level, rows].astype(jnp.float32)) * factor

        for j in range(part):
            for r in range(0, nx, chunk):
                pad[pl.ds(edge + r, chunk)] = both(oc, pc, j, pl.ds(r, chunk), scale)
            for r in range(0, nx, chunk):
                rows = pl.ds(r, chunk)
                mid = pad[pl.ds(edge + r, chunk)]
                beside = both(om, pm, 0, rows, low) if j == 0 else both(oc, pc, j - 1, rows, scale)
                beside = beside + (both(op, pp, 0, rows, high) if j == part - 1 else both(oc, pc, j + 1, rows, scale))
                beside = beside + pad[pl.ds(edge + r - 1, chunk)] + pad[pl.ds(edge + r + 1, chunk)]
                beside = beside + jnp.where(lane > 0, pltpu.roll(mid, 1, 1), 0.0)
                beside = beside + jnp.where(lane < ny - 1, pltpu.roll(mid, ny - 1, 1), 0.0)
                outs[j][0, rows] = 6.0 * mid - beside

    def outer(shift):
        def index(h, core):
            return (jnp.clip((2 * h + core[0]) * part + shift, 0, depth - 1), 0, 0)

        return pl.BlockSpec((1, nx, ny), index)

    centre = pl.BlockSpec((part, nx, ny), lambda h, core: (2 * h + core[0], 0, 0))
    specs = [outer(-1), centre, outer(part)]
    return pl.pallas_call(
        kernel,
        grid_spec=pltpu.PrefetchScalarGridSpec(
            num_scalar_prefetch=1,
            grid=(groups // 2,),
            in_specs=specs + specs,
            out_specs=[pl.BlockSpec((1, nx, ny), lambda h, core: (h, 0, 0))] * part,
            scratch_shapes=[pltpu.VMEM((nx + 2 * edge, ny), jnp.float32)],
        ),
        out_shape=[jax.ShapeDtypeStruct((groups // 2, nx, ny), jnp.float32)] * part,
        name="filter_pair",
    )(core, own, own, own, other, other, other)


def body(partials):
    groups = lax.axis_size("shot")
    members = lax.axis_size("tile")
    shots, depth, nx, ny = partials.shape
    part = depth // groups
    rows = nx // members
    own = partials[0]
    other = lax.ppermute(own, "shot", [(i, i ^ 1) for i in range(groups)])
    core = (lax.axis_index("shot") & 1).reshape(1)
    scale = 1.0 / float(groups * members) ** 0.5
    pair = filter_pair(own, other, core, groups, scale)
    sbits = [("shot", b) for b in reversed(range(1, bits_of(groups)))]
    tbits = [("tile", b) for b in reversed(range(bits_of(members)))]
    labels = sbits + ["part"] + tbits + ["rows", "ny"]
    steps = sbits[::-1] + tbits[::-1]
    first, rest = steps[:3], steps[3:]
    colors = part
    shape = (2,) * len(sbits) + (1,) + (2,) * len(tbits) + (rows, ny)
    pieces = [(level.reshape(shape), labels) for level in pair]
    for k in range(len(steps)):
        for c in range(colors):
            order = first[c % 3 :] + first[: c % 3] + rest
            pieces[c] = halve(*pieces[c], order[k])
    return jnp.concatenate([block for block, left in pieces], axis=0)


def solution(mesh):
    return jax.shard_map(
        body,
        mesh=mesh,
        in_specs=(P(("shot", "tile"), None, None, None),),
        out_specs=P("shot", "tile", None),
        check_vma=False,
    )
```
